8 devices in a mesh: fsdp: 8 (over z, y, x, core).
Axes of the slice: x: 2, y: 2, z: 1, core: 2. Of those that a mesh axis runs over, the one named last changes fastest.
Arguments:
- left_mat: bfloat16 [65536, 4096], P('fsdp')
- right_mat: bfloat16 [4096, 4096], P('fsdp')
Outputs:
- output: bfloat16 [65536, 4096], P('fsdp')
All inputs are finite; a program needn't handle non-finite values.
Results may differ from the reference program's by a relative error of at most 0.001.
Values are sent between devices in bfloat16 or wider.
A program may use at most 1 GiB of HBM per device.

```python
import jax
import jax.numpy as jnp

ROWS_TOTAL = 65536
IN_WIDTH = 4096
OUT_WIDTH = 4096


def setup_inputs(seed: int = 0) -> dict:
    base_key = jax.random.key(seed)
    key_left, key_right = jax.random.split(base_key)
    left_vals = jax.random.normal(key_left, (ROWS_TOTAL, IN_WIDTH), jnp.float32)
    right_vals = jax.random.normal(key_right, (IN_WIDTH, OUT_WIDTH), jnp.float32) * (IN_WIDTH ** -0.5)
    return {"left_mat": left_vals.astype(jnp.bfloat16), "right_mat": right_vals.astype(jnp.bfloat16)}


def reference(left_mat, right_mat):
    return jnp.dot(left_mat, right_mat, preferred_element_type=jnp.float32).astype(jnp.bfloat16)
```

```python
import jax
import jax.numpy as jnp
from jax import lax
from jax.experimental import pallas as pl
from jax.experimental.pallas import tpu as pltpu
from jax.sharding import PartitionSpec as P

MESH = pl.DeviceIdType.MESH
BM = 1024
CW = 256
JW = 512
F32 = jnp.float32
BF16 = jnp.bfloat16

KP, KX, KY, KXP, KYP, KDY, KDX, KDYP, KDXP = range(9)


def _gather_kernel(n1, a_hbm, b_hbm, c1_hbm, bh_hbm, bv, abuf, obuf, acc, own, ssem, rsem, asem, osem, lsem):
    m_rows, k_all = a_hbm.shape
    depth, n_all = b_hbm.shape
    nm = m_rows // BM
    pieces = n_all // CW
    nv = n1 // CW
    slab = 2 * depth
    half = depth // 2

    me = lax.axis_index("fsdp")
    chip = me // 2
    core = me % 2
    chip_x = chip + 1 - 2 * (chip % 2)
    chip_y = (chip + 2) % 4
    chip_d = 3 - chip
    partner = chip * 2 + 1 - core
    dev_x = chip_x * 2 + core
    dev_y = chip_y * 2 + core

    def chip_at(r):
        return (chip, chip_x, chip_y, chip_d)[r]

    barrier = pltpu.get_barrier_semaphore()
    for dev in (partner, dev_x, dev_y):
        pl.semaphore_signal(barrier, inc=1, device_id=(dev,), device_id_type=MESH)

    own_v = pltpu.make_async_copy(
        b_hbm.at[:, pl.ds(0, n1)], bv.at[pl.ds(pl.multiple_of(core * depth, depth), depth), :], lsem.at[0])
    own_h_in = pltpu.make_async_copy(b_hbm.at[:, pl.ds(n1, n_all - n1)], own, lsem.at[1])
    own_h_out = pltpu.make_async_copy(own, bh_hbm.at[pl.ds(pl.multiple_of(me * depth, depth), depth), :], lsem.at[2])

    def a_copy(m, r, slot, place):
        q = chip_at(r)
        return pltpu.make_async_copy(
            a_hbm.at[pl.ds(pl.multiple_of(m * BM, BM), BM), pl.ds(pl.multiple_of(q * slab, slab), slab)],
            abuf.at[slot, :, pl.ds(pl.multiple_of(place * slab, slab), slab)],
            asem.at[slot, place],
        )

    own_v.start()
    own_h_in.start()
    for m in range(8):
        a_copy(m, 0, m % 2, m // 2).start()

    pl.semaphore_wait(barrier, 3)

    def copy(kind, t, in_v):
        cols_b = pl.ds(pl.multiple_of(t * CW, CW), CW)
        buf = bv if in_v else bh_hbm
        cols = cols_b if in_v else pl.ds(pl.multiple_of((t - nv) * CW, CW), CW)

        def rows(r, c, first, size):
            base = (2 * r + c) if in_v else (2 * chip_at(r) + c)
            return pl.ds(pl.multiple_of(base * depth + first, half), size)

        own_src = b_hbm.at[:, cols_b]
        at = lambda r, c, first=0, size=depth: buf.at[rows(r, c, first, size), cols]
        if kind == KP:
            src, dst, dev = own_src, at(0, core), partner
        elif kind == KX:
            src, dst, dev = own_src, (at(1, core) if in_v else at(0, core)), dev_x
        elif kind == KY:
            src, dst, dev = own_src, (at(2, core) if in_v else at(0, core)), dev_y
        elif kind == KXP:
            src, dst, dev = at(1, core), at(1, core), partner
        elif kind == KYP:
            src, dst, dev = at(2, core), at(2, core), partner
        elif kind == KDY:
            src, dst, dev = at(1, core, 0, half), (at(3, core, 0, half) if in_v else at(1, core, 0, half)), dev_y
        elif kind == KDX:
            src, dst, dev = at(2, core, half, half), (at(3, core, half, half) if in_v else at(2, core, half, half)), dev_x
        elif kind == KDYP:
            src, dst, dev = at(3, core, 0, half), at(3, core, 0, half), partner
        else:
            src, dst, dev = at(3, core, half, half), at(3, core, half, half), partner
        return pltpu.make_async_remote_copy(
            src_ref=src, dst_ref=dst, send_sem=ssem.at[kind, t], recv_sem=rsem.at[kind, t],
            device_id=(dev,), device_id_type=MESH)

    def each(t, body):
        if isinstance(t, int):
            if 0 <= t < pieces:
                body(t < nv)
            return

        @pl.when(t < nv)
        def _():
            body(True)

        @pl.when(jnp.logical_and(t >= nv, t < pieces))
        def _():
            body(False)

    def stage_a(t):
        def body(in_v):
            for kind in (KX, KY, KP):
                copy(kind, t, in_v).start()
        each(t, body)

    def stage_b(t):
        def body(in_v):
            copy(KX, t, in_v).wait_recv()
            copy(KDY, t, in_v).start()
            copy(KXP, t, in_v).start()
            copy(KY, t, in_v).wait_recv()
            copy(KDX, t, in_v).start()
            copy(KYP, t, in_v).start()
        each(t, body)

    def stage_c(t):
        def body(in_v):
            copy(KDY, t, in_v).wait_recv()
            copy(KDYP, t, in_v).start()
            copy(KDX, t, in_v).wait_recv()
            copy(KDXP, t, in_v).start()
        each(t, body)

    def landed(t, kinds):
        each(t, lambda in_v: [copy(kind, t, in_v).wait_recv() for kind in kinds])

    def out_copy(m, j, slot):
        return pltpu.make_async_copy(
            obuf.at[slot],
            c1_hbm.at[pl.ds(pl.multiple_of(m * BM, BM), BM), pl.ds(pl.multiple_of(j * JW, JW), JW)],
            osem.at[slot])

    def dot(x, y):
        return jnp.dot(x, y, preferred_element_type=F32)

    stage_a(0)
    stage_a(1)
    own_v.wait()
    landed(0, (KP,))
    landed(1, (KP,))

    def g0(m, carry):
        slot, place = m % 2, m // 2
        a_copy(m, 0, slot, place).wait()

        @pl.when(m == 5)
        def _():
            stage_b(0)

        @pl.when(m == 7)
        def _():
            for r in (1, 2):
                a_copy(0, r, 0, r).start()

        acc[pl.ds(pl.multiple_of(m * BM, BM), BM), :] = dot(
            abuf[slot, :, pl.ds(pl.multiple_of(place * slab, slab), slab)], bv[0:slab, 0:JW])
        return carry

    lax.fori_loop(0, nm, g0, 0)
    stage_b(1)
    stage_a(2)
    landed(0, (KXP, KYP))
    landed(1, (KXP, KYP))

    def g1(m, carry):
        slot = m % 2
        for r in (1, 2):
            a_copy(m, r, slot, r).wait()

        @pl.when(m < nm - 1)
        def _():
            for r in (1, 2):
                a_copy(m + 1, r, 1 - slot, r).start()

        @pl.when(m == 3)
        def _():
            stage_c(0)
            stage_a(3)

        @pl.when(m == 6)
        def _():
            stage_c(1)
            stage_b(2)
            stage_a(4)
            for i in range(4):
                a_copy(i, 3, i % 2, (3, 0)[i // 2]).start()

        @pl.when(m == 7)
        def _():
            a_copy(4, 3, 0, 1).start()
        rows = pl.ds(pl.multiple_of(m * BM, BM), BM)
        acc[rows, :] += dot(abuf[slot, :, slab:3 * slab], bv[slab:3 * slab, 0:JW])
        return carry

    lax.fori_loop(0, nm, g1, 0)
    own_h_in.wait()
    own_h_out.start()
    landed(0, (KDYP, KDXP))
    landed(1, (KDYP, KDXP))
    a_copy(5, 3, 1, 1).start()
    a_copy(6, 3, 0, 2).start()
    a_copy(7, 3, 1, 2).start()

    def g2(m, carry):
        slot, place = m % 2, (3 + m // 2) % 4
        a_copy(m, 3, slot, place).wait()

        @pl.when(m == 3)
        def _():
            a_copy(0, 3, 0, 3).start()
            a_copy(0, 0, 0, 0).start()

        @pl.when(m == 5)
        def _():
            a_copy(0, 1, 0, 1).start()
            stage_b(3)
            stage_a(5)
            stage_c(2)

        @pl.when(m == 7)
        def _():
            a_copy(0, 2, 0, 2).start()

        @pl.when(m >= 2)
        def _():
            out_copy(m - 2, 0, slot).wait()
        rows = pl.ds(pl.multiple_of(m * BM, BM), BM)
        obuf[slot] = (acc[rows, :] + dot(abuf[slot, :, pl.ds(pl.multiple_of(place * slab, slab), slab)],
                                         bv[3 * slab:, 0:JW])).astype(BF16)
        out_copy(m, 0, slot).start()
        return carry

    lax.fori_loop(0, nm, g2, 0)

    jobs = n1 // JW
    steps = nm * (jobs - 1)

    def step(s, carry):
        m, j, slot = s % nm, 1 + s // nm, s % 2
        for r in range(4):
            a_copy(m, r, slot, r).wait()

        @pl.when(s < steps - 1)
        def _():
            for r in range(4):
                a_copy((s + 1) % nm, r, 1 - slot, r).start()

        @pl.when(s % 2 == 0)
        def _():
            u = s // 2
            stage_b(4 + u)
            stage_a(6 + u)
            stage_c(3 + u)

        @pl.when(m == 0)
        def _():
            for i in range(2):
                for kind in (KP, KXP, KYP, KDYP, KDXP):
                    copy(kind, 2 * j + i, True).wait_recv()

        out_copy(m, j, slot).wait()
        obuf[slot] = dot(abuf[slot], bv[:, pl.ds(pl.multiple_of(j * JW, JW), JW)]).astype(BF16)
        out_copy(m, j, slot).start()
        return carry

    lax.fori_loop(0, steps, step, 0)
    for t in range(4 + steps // 2, pieces):
        stage_b(t)
    for t in range(3 + steps // 2, pieces):
        stage_c(t)

    def rest(t, carry):
        for kind in (KP, KXP, KYP, KDYP, KDXP):
            copy(kind, t, False).wait_recv()
        return carry

    lax.fori_loop(nv, pieces, rest, 0)

    def sent(in_v):
        def body(t, carry):
            for kind in range(9):
                copy(kind, t, in_v).wait_send()
            return carry
        return body

    lax.fori_loop(0, nv, sent(True), 0)
    lax.fori_loop(nv, pieces, sent(False), 0)
    own_h_out.wait()
    for slot in range(2):
        out_copy(0, 0, slot).wait()


def _rest_kernel(n1, bn, a_ref, b_ref, c1_hbm, c_hbm, obuf, cbuf, osem, isem, xsem):
    n, m = pl.program_id(0), pl.program_id(1)
    nm = pl.num_programs(1)
    steps = pl.num_programs(0) * nm
    s = n * nm + m
    slot = s % 2
    rows = c1_hbm.shape[0] // (2 * nm)

    def take(i, k):
        return pltpu.make_async_copy(c1_hbm.at[pl.ds(pl.multiple_of(i * rows, rows), rows), :], cbuf.at[k], isem.at[k])

    def put(i, k):
        return pltpu.make_async_copy(
            cbuf.at[k], c_hbm.at[pl.ds(pl.multiple_of(i * rows, rows), rows), pl.ds(0, n1)], xsem.at[k])

    def out(k):
        return pltpu.make_async_copy(
            obuf.at[k],
            c_hbm.at[pl.ds(pl.multiple_of(m * BM, BM), BM), pl.ds(pl.multiple_of(n1 + n * bn, bn), bn)],
            osem.at[k])

    @pl.when(s == 0)
    def _():
        take(0, 0).start()

    take(s, slot).wait()
    put(s, slot).start()

    @pl.when(s >= 1)
    def _():
        put(s - 1, 1 - slot).wait()

    @pl.when(s < steps - 1)
    def _():
        take(s + 1, 1 - slot).start()

    @pl.when(s >= 2)
    def _():
        out(slot).wait()

    obuf[slot] = jnp.dot(a_ref[...], b_ref[...], preferred_element_type=F32).astype(BF16)
    out(slot).start()

    @pl.when(s == steps - 1)
    def _():
        put(s, slot).wait()
        out(1 - slot).wait()
        out(slot).wait()


def solution(mesh):
    def local_fn(a, b):
        m_rows, k_all = a.shape
        depth, n_all = b.shape
        n1 = n_all // 2
        pieces = n_all // CW
        any_spec = pl.BlockSpec(memory_space=pl.ANY)
        c1, bh = pl.pallas_call(
            lambda *refs: _gather_kernel(n1, *refs),
            out_shape=(jax.ShapeDtypeStruct((m_rows, n1), BF16), jax.ShapeDtypeStruct((k_all, n_all - n1), BF16)),
            in_specs=[any_spec, any_spec],
            out_specs=(any_spec, any_spec),
            scratch_shapes=[
                pltpu.VMEM((k_all, n1), BF16),
                pltpu.VMEM((2, BM, k_all), BF16),
                pltpu.VMEM((2, BM, JW), BF16),
                pltpu.VMEM((m_rows, JW), F32),
                pltpu.VMEM((depth, n_all - n1), BF16),
                pltpu.SemaphoreType.DMA((9, pieces)),
                pltpu.SemaphoreType.DMA((9, pieces)),
                pltpu.SemaphoreType.DMA((2, 4)),
                pltpu.SemaphoreType.DMA((2,)),
                pltpu.SemaphoreType.DMA((3,)),
            ],
            compiler_params=pltpu.CompilerParams(
                collective_id=0, has_side_effects=True, vmem_limit_bytes=63 * 1024 * 1024),
            cost_estimate=pl.CostEstimate(
                flops=2 * m_rows * k_all * n1, bytes_accessed=6 * m_rows * k_all, transcendentals=0),
            name="gather_half",
        )(a, b)
        bn = 1024
        nm = m_rows // BM
        return pl.pallas_call(
            lambda *refs: _rest_kernel(n1, bn, *refs),
            grid=((n_all - n1) // bn, nm),
            out_shape=jax.ShapeDtypeStruct((m_rows, n_all), BF16),
            in_specs=[
                pl.BlockSpec((BM, k_all), lambda n, m: (m, 0)),
                pl.BlockSpec((k_all, bn), lambda n, m: (0, n)),
                any_spec,
            ],
            out_specs=any_spec,
            scratch_shapes=[
                pltpu.VMEM((2, BM, bn), BF16),
                pltpu.VMEM((2, m_rows // (2 * nm), n1), BF16),
                pltpu.SemaphoreType.DMA((2,)),
                pltpu.SemaphoreType.DMA((2,)),
                pltpu.SemaphoreType.DMA((2,)),
            ],
            compiler_params=pltpu.CompilerParams(vmem_limit_bytes=60 * 1024 * 1024),
            cost_estimate=pl.CostEstimate(
                flops=2 * m_rows * k_all * (n_all - n1), bytes_accessed=6 * m_rows * k_all, transcendentals=0),
            name="rest",
        )(a, bh, c1)

    spec = P("fsdp", None)
    return jax.shard_map(local_fn, mesh=mesh, in_specs=(spec, spec), out_specs=spec, check_vma=False)
```

```python
import jax
import jax.numpy as jnp
from jax import lax
from jax.experimental import pallas as pl
from jax.experimental.pallas import tpu as pltpu
from jax.sharding import PartitionSpec as P

MESH = pl.DeviceIdType.MESH
BM = 1024
CW = 256
JW = 512
F32 = jnp.float32
BF16 = jnp.bfloat16

KP, KX, KY, KXP, KYP, KDY, KDX, KDYP, KDXP = range(9)


def _gather_kernel(n1, a_hbm, b_hbm, c1_hbm, bh_hbm, bv, abuf, obuf, acc, ssem, rsem, asem, osem, lsem):
    m_rows, k_all = a_hbm.shape
    depth, n_all = b_hbm.shape
    nm = m_rows // BM
    pieces = n_all // CW
    nv = n1 // CW
    slab = 2 * depth
    half = depth // 2

    me = lax.axis_index("fsdp")
    chip = me // 2
    core = me % 2
    chip_x = chip + 1 - 2 * (chip % 2)
    chip_y = (chip + 2) % 4
    chip_d = 3 - chip
    partner = chip * 2 + 1 - core
    dev_x = chip_x * 2 + core
    dev_y = chip_y * 2 + core

    def chip_at(r):
        return (chip, chip_x, chip_y, chip_d)[r]

    barrier = pltpu.get_barrier_semaphore()
    for dev in (partner, dev_x, dev_y):
        pl.semaphore_signal(barrier, inc=1, device_id=(dev,), device_id_type=MESH)

    own_v = pltpu.make_async_copy(
        b_hbm.at[:, pl.ds(0, n1)], bv.at[pl.ds(pl.multiple_of(core * depth, depth), depth), :], lsem.at[0])
    wide = n1 - 2 * JW

    def own_h(k, out):
        col = pl.ds(k * wide, wide)
        stop = obuf.at[k, pl.ds(0, depth), :]
        if out:
            rows = pl.ds(pl.multiple_of(me * depth, depth), depth)
            return pltpu.make_async_copy(stop, bh_hbm.at[rows, col], lsem.at[3 + k])
        return pltpu.make_async_copy(b_hbm.at[:, pl.ds(n1 + k * wide, wide)], stop, lsem.at[1 + k])

    def a_copy(m, r, slot, place):
        q = chip_at(r)
        return pltpu.make_async_copy(
            a_hbm.at[pl.ds(pl.multiple_of(m * BM, BM), BM), pl.ds(pl.multiple_of(q * slab, slab), slab)],
            abuf.at[slot, :, pl.ds(pl.multiple_of(place * slab, slab), slab)],
            asem.at[slot, place],
        )

    own_v.start()
    for m in range(8):
        a_copy(m, 0, m % 2, m // 2).start()
    for k in range(2):
        own_h(k, False).start()

    pl.semaphore_wait(barrier, 3)

    def copy(kind, t, in_v):
        cols_b = pl.ds(pl.multiple_of(t * CW, CW), CW)
        buf = bv if in_v else bh_hbm
        cols = cols_b if in_v else pl.ds(pl.multiple_of((t - nv) * CW, CW), CW)

        def rows(r, c, first, size):
            base = (2 * r + c) if in_v else (2 * chip_at(r) + c)
            return pl.ds(pl.multiple_of(base * depth + first, half), size)

        own_src = b_hbm.at[:, cols_b]
        at = lambda r, c, first=0, size=depth: buf.at[rows(r, c, first, size), cols]
        if kind == KP:
            src, dst, dev = own_src, at(0, core), partner
        elif kind == KX:
            src, dst, dev = own_src, (at(1, core) if in_v else at(0, core)), dev_x
        elif kind == KY:
            src, dst, dev = own_src, (at(2, core) if in_v else at(0, core)), dev_y
        elif kind == KXP:
            src, dst, dev = at(1, core), at(1, core), partner
        elif kind == KYP:
            src, dst, dev = at(2, core), at(2, core), partner
        elif kind == KDY:
            src, dst, dev = at(1, core, 0, half), (at(3, core, 0, half) if in_v else at(1, core, 0, half)), dev_y
        elif kind == KDX:
            src, dst, dev = at(2, core, half, half), (at(3, core, half, half) if in_v else at(2, core, half, half)), dev_x
        elif kind == KDYP:
            src, dst, dev = at(3, core, 0, half), at(3, core, 0, half), partner
        else:
            src, dst, dev = at(3, core, half, half), at(3, core, half, half), partner
        return pltpu.make_async_remote_copy(
            src_ref=src, dst_ref=dst, send_sem=ssem.at[kind, t], recv_sem=rsem.at[kind, t],
            device_id=(dev,), device_id_type=MESH)

    def each(t, body):
        if isinstance(t, int):
            if 0 <= t < pieces:
                body(t < nv)
            return

        @pl.when(t < nv)
        def _():
            body(True)

        @pl.when(jnp.logical_and(t >= nv, t < pieces))
        def _():
            body(False)

    def stage_a(t):
        def body(in_v):
            for kind in (KP, KX, KY):
                copy(kind, t, in_v).start()
        each(t, body)

    def stage_b(t):
        def body(in_v):
            copy(KX, t, in_v).wait_recv()
            copy(KDY, t, in_v).start()
            copy(KXP, t, in_v).start()
            copy(KY, t, in_v).wait_recv()
            copy(KDX, t, in_v).start()
            copy(KYP, t, in_v).start()
        each(t, body)

    def stage_c(t):
        def body(in_v):
            copy(KDY, t, in_v).wait_recv()
            copy(KDYP, t, in_v).start()
            copy(KDX, t, in_v).wait_recv()
            copy(KDXP, t, in_v).start()
        each(t, body)

    def landed(t, kinds):
        each(t, lambda in_v: [copy(kind, t, in_v).wait_recv() for kind in kinds])

    def out_copy(m, col, width, slot):
        return pltpu.make_async_copy(
            obuf.at[slot, :, pl.ds(0, width)],
            c1_hbm.at[pl.ds(pl.multiple_of(m * BM, BM), BM), pl.ds(col, width)],
            osem.at[slot])

    def dot(x, y):
        return jnp.dot(x, y, preferred_element_type=F32)

    def pair(i):
        return pl.ds(pl.multiple_of(i * 2 * BM, 2 * BM), 2 * BM)

    def pair_of(place, width):
        x = abuf[:, :, pl.ds(pl.multiple_of(place * slab, slab), width)]
        return x.reshape(2 * BM, width)

    stage_a(0)
    stage_a(1)
    own_v.wait()
    landed(0, (KP,))
    landed(1, (KP,))

    def g0(i, carry):
        for slot in range(2):
            a_copy(2 * i + slot, 0, slot, i).wait()

        @pl.when(i == 2)
        def _():
            for slot in range(2):
                a_copy(slot, 1, slot, 0).start()
                a_copy(slot, 2, slot, 1).start()

        acc[pair(i), :] = dot(pair_of(i, slab), bv[0:slab, 0:JW])
        return carry

    lax.fori_loop(0, nm // 2, g0, 0)
    for k in range(2):
        own_h(k, False).wait()
        own_h(k, True).start()
    stage_b(0)
    stage_b(1)
    stage_a(2)
    stage_a(3)
    landed(0, (KXP, KYP))
    landed(1, (KXP, KYP))

    def g1(i, carry):
        place = 2 * (i % 2)
        for slot in range(2):
            a_copy(2 * i + slot, 1, slot, place).wait()
            a_copy(2 * i + slot, 2, slot, place + 1).wait()

        @pl.when(i < nm // 2 - 1)
        def _():
            for slot in range(2):
                a_copy(2 * i + 2 + slot, 1, slot, 2 - place).start()
                a_copy(2 * i + 2 + slot, 2, slot, 3 - place).start()

        @pl.when(i == 1)
        def _():
            stage_c(0)
            stage_c(1)

        @pl.when(i == 3)
        def _():
            stage_b(2)
            stage_a(4)
            for slot in range(2):
                a_copy(slot, 3, slot, 0).start()
                a_copy(2 + slot, 3, slot, 1).start()

        acc[pair(i), :] += dot(pair_of(place, 2 * slab), bv[slab:3 * slab, 0:JW])
        return carry

    lax.fori_loop(0, nm // 2, g1, 0)
    landed(0, (KDYP, KDXP))
    landed(1, (KDYP, KDXP))
    stage_b(3)
    stage_a(5)
    stage_c(2)
    for k in range(2):
        own_h(k, True).wait()

    def g2(i, carry):
        for slot in range(2):
            a_copy(2 * i + slot, 3, slot, i).wait()

        @pl.when(i == 0)
        def _():
            for slot in range(2):
                a_copy(4 + slot, 3, slot, 2).start()
            a_copy(6, 3, 1, 3).start()
            a_copy(0, 3, 0, 3).start()

        @pl.when(i == 1)
        def _():
            a_copy(0, 0, 0, 0).start()
            a_copy(7, 3, 1, 0).start()

        @pl.when(i == 2)
        def _():
            a_copy(0, 1, 0, 1).start()

        @pl.when(i >= 1)
        def _():
            for slot in range(2):
                out_copy(2 * i - 2 + slot, 0, JW, slot).wait()

        res = (acc[pair(i), :] + dot(pair_of(i, slab), bv[3 * slab:, 0:JW])).astype(BF16)
        obuf[:, :, 0:JW] = res.reshape(2, BM, JW)
        for slot in range(2):
            out_copy(2 * i + slot, 0, JW, slot).start()
        return carry

    lax.fori_loop(0, nm // 2 - 1, g2, 0)
    a_copy(0, 2, 0, 2).start()
    stage_b(4)
    stage_a(6)

    def g2_last(m, carry):
        slot, place = m % 2, 3 * (7 - m)
        a_copy(m, 3, 1, place).wait()
        out_copy(m - 2, 0, JW, slot).wait()
        rows = pl.ds(pl.multiple_of(m * BM, BM), BM)
        obuf[slot, :, 0:JW] = (acc[rows, :] + dot(
            abuf[1, :, pl.ds(pl.multiple_of(place * slab, slab), slab)], bv[3 * slab:, 0:JW])).astype(BF16)
        out_copy(m, 0, JW, slot).start()
        return carry

    lax.fori_loop(nm - 2, nm, g2_last, 0)

    def tiles(s, m, last):
        slot = s % 2
        for r in range(4):
            a_copy(m, r, slot, r).wait()

        def ahead():
            for r in range(4):
                a_copy((m + 1) % nm, r, 1 - slot, r).start()

        if last is None:
            ahead()
        else:
            pl.when(jnp.logical_not(last))(ahead)
        return slot

    def job1(m, carry):
        slot = tiles(m, m, None)
        h = m // 2

        @pl.when(m % 2 == 0)
        def _():
            stage_c(3 + h)

        @pl.when(m % 2 == 1)
        def _():
            @pl.when(m < nm - 1)
            def _():
                stage_b(5 + h)
            stage_a(7 + h)

        @pl.when(m == nm - 1)
        def _():
            stage_c(7)

        @pl.when(m == 0)
        def _():
            for t in (2, 3):
                landed(t, (KP, KXP, KYP, KDYP, KDXP))

        out_copy(m, JW, JW, slot).wait()
        obuf[slot, :, 0:JW] = dot(abuf[slot], bv[:, JW:2 * JW]).astype(BF16)
        out_copy(m, JW, JW, slot).start()
        return carry

    lax.fori_loop(0, nm, job1, 0)
    for t in range(4, 8):
        landed(t, (KP, KXP, KYP, KDYP, KDXP))
    def job2(m, carry):
        slot = tiles(m, m, m == nm - 1)
        stage_b(8 + m)
        stage_a(11 + m)

        @pl.when(m >= 2)
        def _():
            stage_c(6 + m)

        @pl.when(m == nm - 1)
        def _():
            stage_c(14)

        @pl.when(m < 2)
        def _():
            out_copy(m, JW, JW, slot).wait()

        @pl.when(m >= 2)
        def _():
            out_copy(m, 2 * JW, wide, slot).wait()

        obuf[slot] = dot(abuf[slot], bv[:, 2 * JW:]).astype(BF16)
        out_copy(m, 2 * JW, wide, slot).start()
        return carry

    lax.fori_loop(0, nm, job2, 0)
    stage_c(15)

    def rest(t, carry):
        for kind in (KP, KXP, KYP, KDYP, KDXP):
            copy(kind, t, False).wait_recv()
        return carry

    lax.fori_loop(nv, pieces, rest, 0)

    def sent(in_v):
        def body(t, carry):
            for kind in range(9):
                copy(kind, t, in_v).wait_send()
            return carry
        return body

    lax.fori_loop(0, nv, sent(True), 0)
    lax.fori_loop(nv, pieces, sent(False), 0)
    for slot in range(2):
        out_copy(0, 2 * JW, wide, slot).wait()


def _rest_kernel(n1, bn, a_hbm, b_hbm, c1_hbm, c_hbm, abuf, bbuf, obuf, acc, cbuf, asem, bsem, osem, isem, xsem):
    m_rows, k_all = a_hbm.shape
    nm = m_rows // BM
    steps = nm * (b_hbm.shape[1] // bn)
    rows = m_rows // steps
    slab = k_all // 4

    def take(i, k):
        return pltpu.make_async_copy(c1_hbm.at[pl.ds(pl.multiple_of(i * rows, rows), rows), :], cbuf.at[k], isem.at[k])

    def put(i, k):
        return pltpu.make_async_copy(
            cbuf.at[k], c_hbm.at[pl.ds(pl.multiple_of(i * rows, rows), rows), pl.ds(0, n1)], xsem.at[k])

    def out(s, k):
        m, n = s % nm, s // nm
        return pltpu.make_async_copy(
            obuf.at[k],
            c_hbm.at[pl.ds(pl.multiple_of(m * BM, BM), BM), pl.ds(pl.multiple_of(n1 + n * bn, bn), bn)],
            osem.at[k])

    def a_slab(r):
        return pltpu.make_async_copy(
            a_hbm.at[pl.ds(0, BM), pl.ds(pl.multiple_of(r * slab, slab), slab)],
            abuf.at[0, :, pl.ds(pl.multiple_of(r * slab, slab), slab)], asem.at[2 + r])

    def b_slab(r):
        return pltpu.make_async_copy(
            b_hbm.at[pl.ds(pl.multiple_of(r * slab, slab), slab), pl.ds(0, bn)],
            bbuf.at[0, pl.ds(pl.multiple_of(r * slab, slab), slab), :], bsem.at[1 + r])

    def a_tile(s, k):
        return pltpu.make_async_copy(
            a_hbm.at[pl.ds(pl.multiple_of((s % nm) * BM, BM), BM), :], abuf.at[k], asem.at[k])

    b_next = pltpu.make_async_copy(b_hbm.at[:, pl.ds(bn, bn)], bbuf.at[1], bsem.at[0])

    for r in range(4):
        a_slab(r).start()
        b_slab(r).start()
    a_tile(1, 1).start()
    take(0, 0).start()
    acc[...] = jnp.zeros_like(acc)

    def part(r):
        a_slab(r).wait()
        b_slab(r).wait()
        cols = pl.ds(pl.multiple_of(r * slab, slab), slab)
        return jnp.dot(abuf[0, :, cols], bbuf[0, cols, :], preferred_element_type=F32)

    def first(r, carry):
        acc[...] += part(r)
        return carry

    lax.fori_loop(0, 3, first, 0)
    obuf[0] = (acc[...] + part(3)).astype(BF16)
    out(0, 0).start()
    take(0, 0).wait()
    put(0, 0).start()

    def step(s, carry):
        k, c = s % 2, s % 3
        a_tile(s, k).wait()

        @pl.when(s < steps - 1)
        def _():
            a_tile(s + 1, 1 - k).start()

        @pl.when(s == 1)
        def _():
            b_next.start()

        @pl.when(s == nm)
        def _():
            b_next.wait()

        @pl.when(jnp.logical_and(s >= 3, s < steps - 1))
        def _():
            put(s - 3, c).wait()

        @pl.when(s < steps - 1)
        def _():
            take(s, c).start()

        @pl.when(s == steps - 2)
        def _():
            put(steps - 4, (steps - 1) % 3).wait()
            take(steps - 1, (steps - 1) % 3).start()

        @pl.when(s >= 2)
        def _():
            out(s - 2, k).wait()

        obuf[k] = jnp.dot(abuf[k], bbuf[s // nm], preferred_element_type=F32).astype(BF16)
        out(s, k).start()

        @pl.when(s < steps - 1)
        def _():
            take(s, c).wait()
            put(s, c).start()

        @pl.when(s == steps - 2)
        def _():
            take(steps - 1, (steps - 1) % 3).wait()
            put(steps - 1, (steps - 1) % 3).start()
        return carry

    lax.fori_loop(1, steps, step, 0)
    for i in range(steps - 3, steps):
        put(i, i % 3).wait()
    for s in (steps - 2, steps - 1):
        out(s, s % 2).wait()


def solution(mesh):
    def local_fn(a, b):
        m_rows, k_all = a.shape
        depth, n_all = b.shape
        n1 = n_all // 2
        pieces = n_all // CW
        any_spec = pl.BlockSpec(memory_space=pl.ANY)
        c1, bh = pl.pallas_call(
            lambda *refs: _gather_kernel(n1, *refs),
            out_shape=(jax.ShapeDtypeStruct((m_rows, n1), BF16), jax.ShapeDtypeStruct((k_all, n_all - n1), BF16)),
            in_specs=[any_spec, any_spec],
            out_specs=(any_spec, any_spec),
            scratch_shapes=[
                pltpu.VMEM((k_all, n1), BF16),
                pltpu.VMEM((2, BM, k_all), BF16),
                pltpu.VMEM((2, BM, n1 - 2 * JW), BF16),
                pltpu.VMEM((m_rows, JW), F32),
                pltpu.SemaphoreType.DMA((9, pieces)),
                pltpu.SemaphoreType.DMA((9, pieces)),
                pltpu.SemaphoreType.DMA((2, 4)),
                pltpu.SemaphoreType.DMA((2,)),
                pltpu.SemaphoreType.DMA((5,)),
            ],
            compiler_params=pltpu.CompilerParams(
                collective_id=0, has_side_effects=True, vmem_limit_bytes=63 * 1024 * 1024),
            cost_estimate=pl.CostEstimate(
                flops=2 * m_rows * k_all * n1, bytes_accessed=6 * m_rows * k_all, transcendentals=0),
            name="gather_half",
        )(a, b)
        bn = 1024
        nm = m_rows // BM
        return pl.pallas_call(
            lambda *refs: _rest_kernel(n1, bn, *refs),
            out_shape=jax.ShapeDtypeStruct((m_rows, n_all), BF16),
            in_specs=[any_spec, any_spec, any_spec],
            out_specs=any_spec,
            scratch_shapes=[
                pltpu.VMEM((2, BM, k_all), BF16),
                pltpu.VMEM((2, k_all, bn), BF16),
                pltpu.VMEM((2, BM, bn), BF16),
                pltpu.VMEM((BM, bn), F32),
                pltpu.VMEM((3, m_rows // (2 * nm), n1), BF16),
                pltpu.SemaphoreType.DMA((6,)),
                pltpu.SemaphoreType.DMA((5,)),
                pltpu.SemaphoreType.DMA((2,)),
                pltpu.SemaphoreType.DMA((3,)),
                pltpu.SemaphoreType.DMA((3,)),
            ],
            compiler_params=pltpu.CompilerParams(vmem_limit_bytes=63 * 1024 * 1024),
            cost_estimate=pl.CostEstimate(
                flops=2 * m_rows * k_all * (n_all - n1), bytes_accessed=6 * m_rows * k_all, transcendentals=0),
            name="rest",
        )(a, bh, c1)

    spec = P("fsdp", None)
    return jax.shard_map(local_fn, mesh=mesh, in_specs=(spec, spec), out_specs=spec, check_vma=False)
```

```python
import jax
import jax.numpy as jnp
from jax import lax
from jax.experimental import pallas as pl
from jax.experimental.pallas import tpu as pltpu
from jax.sharding import PartitionSpec as P

MESH = pl.DeviceIdType.MESH
BM = 1024
CW = 256
JW = 512
F32 = jnp.float32
BF16 = jnp.bfloat16

KP, KX, KY, KXP, KYP, KDY, KDX, KDYP, KDXP = range(9)


def _gather_kernel(n1, a_hbm, b_hbm, c1_hbm, bh_hbm, bv, abuf, obuf, acc, ssem, rsem, asem, osem, lsem):
    m_rows, k_all = a_hbm.shape
    depth, n_all = b_hbm.shape
    nm = m_rows // BM
    pieces = n_all // CW
    nv = n1 // CW
    slab = 2 * depth
    half = depth // 2

    me = lax.axis_index("fsdp")
    chip = me // 2
    core = me % 2
    chip_x = chip + 1 - 2 * (chip % 2)
    chip_y = (chip + 2) % 4
    chip_d = 3 - chip
    partner = chip * 2 + 1 - core
    dev_x = chip_x * 2 + core
    dev_y = chip_y * 2 + core

    def chip_at(r):
        return (chip, chip_x, chip_y, chip_d)[r]

    barrier = pltpu.get_barrier_semaphore()
    for dev in (partner, dev_x, dev_y):
        pl.semaphore_signal(barrier, inc=1, device_id=(dev,), device_id_type=MESH)

    def own_v(first):
        col, width, k = (0, JW, 0) if first else (JW, n1 - JW, 5)
        rows = pl.ds(pl.multiple_of(core * depth, depth), depth)
        return pltpu.make_async_copy(b_hbm.at[:, pl.ds(col, width)], bv.at[rows, pl.ds(col, width)], lsem.at[k])

    wide = n1 - 2 * JW

    def own_h(k, out):
        col = pl.ds(k * wide, wide)
        stop = obuf.at[k, pl.ds(0, depth), :]
        if out:
            rows = pl.ds(pl.multiple_of(me * depth, depth), depth)
            return pltpu.make_async_copy(stop, bh_hbm.at[rows, col], lsem.at[3 + k])
        return pltpu.make_async_copy(b_hbm.at[:, pl.ds(n1 + k * wide, wide)], stop, lsem.at[1 + k])

    def a_copy(m, r, slot, place):
        q = chip_at(r)
        return pltpu.make_async_copy(
            a_hbm.at[pl.ds(pl.multiple_of(m * BM, BM), BM), pl.ds(pl.multiple_of(q * slab, slab), slab)],
            abuf.at[slot, :, pl.ds(pl.multiple_of(place * slab, slab), slab)],
            asem.at[slot, place],
        )

    own_v(True).start()
    for m in range(2):
        a_copy(m, 0, m % 2, m // 2).start()

    pl.semaphore_wait(barrier, 3)

    def copy(kind, t, in_v):
        cols_b = pl.ds(pl.multiple_of(t * CW, CW), CW)
        buf = bv if in_v else bh_hbm
        cols = cols_b if in_v else pl.ds(pl.multiple_of((t - nv) * CW, CW), CW)

        def rows(r, c, first, size):
            base = (2 * r + c) if in_v else (2 * chip_at(r) + c)
            return pl.ds(pl.multiple_of(base * depth + first, half), size)

        own_src = b_hbm.at[:, cols_b]
        at = lambda r, c, first=0, size=depth: buf.at[rows(r, c, first, size), cols]
        if kind == KP:
            src, dst, dev = own_src, at(0, core), partner
        elif kind == KX:
            src, dst, dev = own_src, (at(1, core) if in_v else at(0, core)), dev_x
        elif kind == KY:
            src, dst, dev = own_src, (at(2, core) if in_v else at(0, core)), dev_y
        elif kind == KXP:
            src, dst, dev = at(1, core), at(1, core), partner
        elif kind == KYP:
            src, dst, dev = at(2, core), at(2, core), partner
        elif kind == KDY:
            src, dst, dev = at(1, core, 0, half), (at(3, core, 0, half) if in_v else at(1, core, 0, half)), dev_y
        elif kind == KDX:
            src, dst, dev = at(2, core, half, half), (at(3, core, half, half) if in_v else at(2, core, half, half)), dev_x
        elif kind == KDYP:
            src, dst, dev = at(3, core, 0, half), at(3, core, 0, half), partner
        else:
            src, dst, dev = at(3, core, half, half), at(3, core, half, half), partner
        return pltpu.make_async_remote_copy(
            src_ref=src, dst_ref=dst, send_sem=ssem.at[kind, t], recv_sem=rsem.at[kind, t],
            device_id=(dev,), device_id_type=MESH)

    def each(t, body):
        if isinstance(t, int):
            if 0 <= t < pieces:
                body(t < nv)
            return

        @pl.when(t < nv)
        def _():
            body(True)

        @pl.when(jnp.logical_and(t >= nv, t < pieces))
        def _():
            body(False)

    def stage_a(t):
        def body(in_v):
            for kind in (KP, KX, KY):
                copy(kind, t, in_v).start()
        each(t, body)

    def stage_b(t):
        def body(in_v):
            copy(KX, t, in_v).wait_recv()
            copy(KDY, t, in_v).start()
            copy(KXP, t, in_v).start()
            copy(KY, t, in_v).wait_recv()
            copy(KDX, t, in_v).start()
            copy(KYP, t, in_v).start()
        each(t, body)

    def stage_c(t):
        def body(in_v):
            copy(KDY, t, in_v).wait_recv()
            copy(KDYP, t, in_v).start()
            copy(KDX, t, in_v).wait_recv()
            copy(KDXP, t, in_v).start()
        each(t, body)

    def landed(t, kinds):
        each(t, lambda in_v: [copy(kind, t, in_v).wait_recv() for kind in kinds])

    def out_copy(m, col, width, slot):
        return pltpu.make_async_copy(
            obuf.at[slot, :, pl.ds(0, width)],
            c1_hbm.at[pl.ds(pl.multiple_of(m * BM, BM), BM), pl.ds(col, width)],
            osem.at[slot])

    def dot(x, y):
        return jnp.dot(x, y, preferred_element_type=F32)

    def pair(i):
        return pl.ds(pl.multiple_of(i * 2 * BM, 2 * BM), 2 * BM)

    def pair_of(place, width):
        x = abuf[:, :, pl.ds(pl.multiple_of(place * slab, slab), width)]
        return x.reshape(2 * BM, width)

    stage_a(0)
    stage_a(1)
    for m in range(2, 8):
        a_copy(m, 0, m % 2, m // 2).start()
    own_v(False).start()
    for k in range(2):
        own_h(k, False).start()
    own_v(True).wait()
    landed(0, (KP,))
    landed(1, (KP,))

    def g0(i, carry):
        for slot in range(2):
            a_copy(2 * i + slot, 0, slot, i).wait()

        @pl.when(i == 2)
        def _():
            for slot in range(2):
                a_copy(slot, 1, slot, 0).start()
                a_copy(slot, 2, slot, 1).start()

        acc[pair(i), :] = dot(pair_of(i, slab), bv[0:slab, 0:JW])
        return carry

    lax.fori_loop(0, nm // 2, g0, 0)
    for k in range(2):
        own_h(k, False).wait()
        own_h(k, True).start()
    stage_b(0)
    stage_b(1)
    stage_a(2)
    stage_a(3)
    landed(0, (KXP, KYP))
    landed(1, (KXP, KYP))

    def g1(i, carry):
        place = 2 * (i % 2)
        for slot in range(2):
            a_copy(2 * i + slot, 1, slot, place).wait()
            a_copy(2 * i + slot, 2, slot, place + 1).wait()

        @pl.when(i < nm // 2 - 1)
        def _():
            for slot in range(2):
                a_copy(2 * i + 2 + slot, 1, slot, 2 - place).start()
                a_copy(2 * i + 2 + slot, 2, slot, 3 - place).start()

        @pl.when(i == 2)
        def _():
            stage_c(0)
            stage_c(1)

        @pl.when(i == 3)
        def _():
            stage_b(2)
            stage_a(4)
            for slot in range(2):
                a_copy(slot, 3, slot, 0).start()
                a_copy(2 + slot, 3, slot, 1).start()

        acc[pair(i), :] += dot(pair_of(place, 2 * slab), bv[slab:3 * slab, 0:JW])
        return carry

    lax.fori_loop(0, nm // 2, g1, 0)
    landed(0, (KDYP, KDXP))
    landed(1, (KDYP, KDXP))
    stage_b(3)
    stage_a(5)
    stage_c(2)
    for k in range(2):
        own_h(k, True).wait()

    def g2(i, carry):
        for slot in range(2):
            a_copy(2 * i + slot, 3, slot, i).wait()

        @pl.when(i == 0)
        def _():
            for slot in range(2):
                a_copy(4 + slot, 3, slot, 2).start()
            a_copy(6, 3, 1, 3).start()
            a_copy(0, 3, 0, 3).start()

        @pl.when(i == 1)
        def _():
            a_copy(0, 0, 0, 0).start()
            a_copy(7, 3, 1, 0).start()

        @pl.when(i == 2)
        def _():
            a_copy(0, 1, 0, 1).start()

        acc[pair(i), :] += dot(pair_of(i, slab), bv[3 * slab:, 0:JW])

        @pl.when(i >= 1)
        def _():
            for slot in range(2):
                out_copy(2 * i - 2 + slot, 0, JW, slot).wait()

        res = acc[pair(i), :].astype(BF16)
        obuf[:, :, 0:JW] = res.reshape(2, BM, JW)
        for slot in range(2):
            out_copy(2 * i + slot, 0, JW, slot).start()
        return carry

    lax.fori_loop(0, nm // 2 - 1, g2, 0)
    a_copy(0, 2, 0, 2).start()
    stage_b(4)
    stage_a(6)

    def g2_last(m, carry):
        slot, place = m % 2, 3 * (7 - m)
        a_copy(m, 3, 1, place).wait()
        rows = pl.ds(pl.multiple_of(m * BM, BM), BM)
        acc[rows, :] += dot(abuf[1, :, pl.ds(pl.multiple_of(place * slab, slab), slab)], bv[3 * slab:, 0:JW])
        out_copy(m - 2, 0, JW, slot).wait()
        obuf[slot, :, 0:JW] = acc[rows, :].astype(BF16)
        out_copy(m, 0, JW, slot).start()
        return carry

    lax.fori_loop(nm - 2, nm, g2_last, 0)

    def tiles(s, m, last):
        slot = s % 2
        for r in range(4):
            a_copy(m, r, slot, r).wait()

        def ahead():
            for r in range(4):
                a_copy((m + 1) % nm, r, 1 - slot, r).start()

        if last is None:
            ahead()
        else:
            pl.when(jnp.logical_not(last))(ahead)
        return slot

    def job1(m, carry):
        slot = tiles(m, m, None)
        h = m // 2

        @pl.when(m % 2 == 0)
        def _():
            stage_c(3 + h)

        @pl.when(m % 2 == 1)
        def _():
            stage_b(5 + h)
            stage_a(7 + h)

        @pl.when(m == nm - 1)
        def _():
            stage_c(7)

        @pl.when(m == 0)
        def _():
            for t in (2, 3):
                landed(t, (KP, KXP, KYP, KDYP, KDXP))

        out_copy(m, JW, JW, slot).wait()
        obuf[slot, :, 0:JW] = dot(abuf[slot], bv[:, JW:2 * JW]).astype(BF16)
        out_copy(m, JW, JW, slot).start()
        return carry

    own_v(False).wait()
    lax.fori_loop(0, nm, job1, 0)
    for t in range(4, 8):
        landed(t, (KP, KXP, KYP, KDYP, KDXP))
    def job2(m, carry):
        slot = tiles(m, m, m == nm - 1)
        stage_b(9 + m)
        stage_a(11 + m)

        @pl.when(m >= 1)
        def _():
            stage_c(7 + m)

        @pl.when(m == nm - 1)
        def _():
            stage_c(15)

        @pl.when(m < 2)
        def _():
            out_copy(m, JW, JW, slot).wait()

        @pl.when(m >= 2)
        def _():
            out_copy(m, 2 * JW, wide, slot).wait()

        obuf[slot] = dot(abuf[slot], bv[:, 2 * JW:]).astype(BF16)
        out_copy(m, 2 * JW, wide, slot).start()
        return carry

    lax.fori_loop(0, nm, job2, 0)

    def rest(t, carry):
        for kind in (KP, KXP, KYP, KDYP, KDXP):
            copy(kind, t, False).wait_recv()
        return carry

    lax.fori_loop(nv, pieces, rest, 0)

    def sent(in_v):
        def body(t, carry):
            for kind in range(9):
                copy(kind, t, in_v).wait_send()
            return carry
        return body

    lax.fori_loop(0, nv, sent(True), 0)
    lax.fori_loop(nv, pieces, sent(False), 0)
    for slot in range(2):
        out_copy(0, 2 * JW, wide, slot).wait()


def _rest_kernel(n1, bn, a_hbm, b_hbm, c1_hbm, c_hbm, abuf, bbuf, obuf, acc, cbuf, asem, bsem, osem, isem, xsem):
    m_rows, k_all = a_hbm.shape
    nm = m_rows // BM
    steps = nm * (b_hbm.shape[1] // bn)
    rows = m_rows // steps
    slab = k_all // 4

    def take(i, k):
        return pltpu.make_async_copy(c1_hbm.at[pl.ds(pl.multiple_of(i * rows, rows), rows), :], cbuf.at[k], isem.at[k])

    def put(i, k):
        return pltpu.make_async_copy(
            cbuf.at[k], c_hbm.at[pl.ds(pl.multiple_of(i * rows, rows), rows), pl.ds(0, n1)], xsem.at[k])

    def out(s, k):
        m, n = s % nm, s // nm
        return pltpu.make_async_copy(
            obuf.at[k],
            c_hbm.at[pl.ds(pl.multiple_of(m * BM, BM), BM), pl.ds(pl.multiple_of(n1 + n * bn, bn), bn)],
            osem.at[k])

    def a_slab(r):
        return pltpu.make_async_copy(
            a_hbm.at[pl.ds(0, BM), pl.ds(pl.multiple_of(r * slab, slab), slab)],
            abuf.at[0, :, pl.ds(pl.multiple_of(r * slab, slab), slab)], asem.at[2 + r])

    def b_slab(r):
        return pltpu.make_async_copy(
            b_hbm.at[pl.ds(pl.multiple_of(r * slab, slab), slab), pl.ds(0, bn)],
            bbuf.at[0, pl.ds(pl.multiple_of(r * slab, slab), slab), :], bsem.at[1 + r])

    def a_tile(s, k):
        return pltpu.make_async_copy(
            a_hbm.at[pl.ds(pl.multiple_of((s % nm) * BM, BM), BM), :], abuf.at[k], asem.at[k])

    b_next = pltpu.make_async_copy(b_hbm.at[:, pl.ds(bn, bn)], bbuf.at[1], bsem.at[0])

    for r in range(4):
        a_slab(r).start()
        b_slab(r).start()
    a_tile(1, 1).start()
    take(0, 0).start()
    acc[...] = jnp.zeros_like(acc)

    def part(r):
        a_slab(r).wait()
        b_slab(r).wait()
        cols = pl.ds(pl.multiple_of(r * slab, slab), slab)
        return jnp.dot(abuf[0, :, cols], bbuf[0, cols, :], preferred_element_type=F32)

    def first(r, carry):
        acc[...] += part(r)
        return carry

    lax.fori_loop(0, 3, first, 0)
    obuf[0] = (acc[...] + part(3)).astype(BF16)
    out(0, 0).start()
    take(0, 0).wait()
    put(0, 0).start()

    def step(s, carry):
        k, c = s % 2, s % 3
        a_tile(s, k).wait()

        @pl.when(s < steps - 1)
        def _():
            a_tile(s + 1, 1 - k).start()

        @pl.when(s == 1)
        def _():
            b_next.start()

        @pl.when(s == nm)
        def _():
            b_next.wait()

        @pl.when(jnp.logical_and(s >= 3, s < steps - 1))
        def _():
            put(s - 3, c).wait()

        @pl.when(s < steps - 1)
        def _():
            take(s, c).start()

        @pl.when(s == steps - 2)
        def _():
            put(steps - 4, (steps - 1) % 3).wait()
            take(steps - 1, (steps - 1) % 3).start()

        @pl.when(s >= 2)
        def _():
            out(s - 2, k).wait()

        obuf[k] = jnp.dot(abuf[k], bbuf[s // nm], preferred_element_type=F32).astype(BF16)
        out(s, k).start()

        @pl.when(s < steps - 1)
        def _():
            take(s, c).wait()
            put(s, c).start()

        @pl.when(s == steps - 2)
        def _():
            take(steps - 1, (steps - 1) % 3).wait()
            put(steps - 1, (steps - 1) % 3).start()
        return carry

    lax.fori_loop(1, steps, step, 0)
    for i in range(steps - 3, steps):
        put(i, i % 3).wait()
    for s in (steps - 2, steps - 1):
        out(s, s % 2).wait()


def solution(mesh):
    def local_fn(a, b):
        m_rows, k_all = a.shape
        depth, n_all = b.shape
        n1 = n_all // 2
        pieces = n_all // CW
        any_spec = pl.BlockSpec(memory_space=pl.ANY)
        c1, bh = pl.pallas_call(
            lambda *refs: _gather_kernel(n1, *refs),
            out_shape=(jax.ShapeDtypeStruct((m_rows, n1), BF16), jax.ShapeDtypeStruct((k_all, n_all - n1), BF16)),
            in_specs=[any_spec, any_spec],
            out_specs=(any_spec, any_spec),
            scratch_shapes=[
                pltpu.VMEM((k_all, n1), BF16),
                pltpu.VMEM((2, BM, k_all), BF16),
                pltpu.VMEM((2, BM, n1 - 2 * JW), BF16),
                pltpu.VMEM((m_rows, JW), F32),
                pltpu.SemaphoreType.DMA((9, pieces)),
                pltpu.SemaphoreType.DMA((9, pieces)),
                pltpu.SemaphoreType.DMA((2, 4)),
                pltpu.SemaphoreType.DMA((2,)),
                pltpu.SemaphoreType.DMA((6,)),
            ],
            compiler_params=pltpu.CompilerParams(
                collective_id=0, has_side_effects=True, vmem_limit_bytes=63 * 1024 * 1024),
            cost_estimate=pl.CostEstimate(
                flops=2 * m_rows * k_all * n1, bytes_accessed=6 * m_rows * k_all, transcendentals=0),
            name="gather_half",
        )(a, b)
        bn = 1024
        nm = m_rows // BM
        return pl.pallas_call(
            lambda *refs: _rest_kernel(n1, bn, *refs),
            out_shape=jax.ShapeDtypeStruct((m_rows, n_all), BF16),
            in_specs=[any_spec, any_spec, any_spec],
            out_specs=any_spec,
            scratch_shapes=[
                pltpu.VMEM((2, BM, k_all), BF16),
                pltpu.VMEM((2, k_all, bn), BF16),
                pltpu.VMEM((2, BM, bn), BF16),
                pltpu.VMEM((BM, bn), F32),
                pltpu.VMEM((3, m_rows // (2 * nm), n1), BF16),
                pltpu.SemaphoreType.DMA((6,)),
                pltpu.SemaphoreType.DMA((5,)),
                pltpu.SemaphoreType.DMA((2,)),
                pltpu.SemaphoreType.DMA((3,)),
                pltpu.SemaphoreType.DMA((3,)),
            ],
            compiler_params=pltpu.CompilerParams(vmem_limit_bytes=63 * 1024 * 1024),
            cost_estimate=pl.CostEstimate(
                flops=2 * m_rows * k_all * (n_all - n1), bytes_accessed=6 * m_rows * k_all, transcendentals=0),
            name="rest",
        )(a, bh, c1)

    spec = P("fsdp", None)
    return jax.shard_map(local_fn, mesh=mesh, in_specs=(spec, spec), out_specs=spec, check_vma=False)
```

```python
import jax
import jax.numpy as jnp
from jax import lax
from jax.experimental import pallas as pl
from jax.experimental.pallas import tpu as pltpu
from jax.sharding import PartitionSpec as P

MESH = pl.DeviceIdType.MESH
BM = 1024
CW = 256
JW = 512
F32 = jnp.float32
BF16 = jnp.bfloat16

KP, KX, KY, KXP, KYP, KDY, KDX, KDYP, KDXP = range(9)


def _gather_kernel(n1, a_hbm, b_hbm, c1_hbm, bh_hbm, bv, abuf, obuf, acc, ssem, rsem, asem, osem, lsem):
    m_rows, k_all = a_hbm.shape
    depth, n_all = b_hbm.shape
    nm = m_rows // BM
    pieces = n_all // CW
    nv = n1 // CW
    slab = 2 * depth
    half = depth // 2

    me = lax.axis_index("fsdp")
    chip = me // 2
    core = me % 2
    chip_x = chip + 1 - 2 * (chip % 2)
    chip_y = (chip + 2) % 4
    chip_d = 3 - chip
    partner = chip * 2 + 1 - core
    dev_x = chip_x * 2 + core
    dev_y = chip_y * 2 + core

    def chip_at(r):
        return (chip, chip_x, chip_y, chip_d)[r]

    barrier = pltpu.get_barrier_semaphore()
    for dev in (partner, dev_x, dev_y):
        pl.semaphore_signal(barrier, inc=1, device_id=(dev,), device_id_type=MESH)

    def own_v(first):
        col, width, k = (0, JW, 0) if first else (JW, n1 - JW, 5)
        rows = pl.ds(pl.multiple_of(core * depth, depth), depth)
        return pltpu.make_async_copy(b_hbm.at[:, pl.ds(col, width)], bv.at[rows, pl.ds(col, width)], lsem.at[k])

    wide = n1 - 2 * JW

    def own_h(k, out):
        col = pl.ds(k * wide, wide)
        stop = obuf.at[k, pl.ds(0, depth), :]
        if out:
            rows = pl.ds(pl.multiple_of(me * depth, depth), depth)
            return pltpu.make_async_copy(stop, bh_hbm.at[rows, col], lsem.at[3 + k])
        return pltpu.make_async_copy(b_hbm.at[:, pl.ds(n1 + k * wide, wide)], stop, lsem.at[1 + k])

    def a_copy(m, r, slot, place):
        q = chip_at(r)
        return pltpu.make_async_copy(
            a_hbm.at[pl.ds(pl.multiple_of(m * BM, BM), BM), pl.ds(pl.multiple_of(q * slab, slab), slab)],
            abuf.at[slot, :, pl.ds(pl.multiple_of(place * slab, slab), slab)],
            asem.at[slot, place],
        )

    own_v(True).start()
    for m in range(2):
        a_copy(m, 0, m % 2, m // 2).start()

    pl.semaphore_wait(barrier, 3)

    def copy(kind, t, in_v):
        cols_b = pl.ds(pl.multiple_of(t * CW, CW), CW)
        buf = bv if in_v else bh_hbm
        cols = cols_b if in_v else pl.ds(pl.multiple_of((t - nv) * CW, CW), CW)

        def rows(r, c, first, size):
            base = (2 * r + c) if in_v else (2 * chip_at(r) + c)
            return pl.ds(pl.multiple_of(base * depth + first, half), size)

        at = lambda r, c, first=0, size=depth: buf.at[rows(r, c, first, size), cols]
        first = isinstance(t, int) and t < JW // CW
        own_src = at(0, core) if first else b_hbm.at[:, cols_b]
        if kind == KP:
            src, dst, dev = own_src, at(0, core), partner
        elif kind == KX:
            src, dst, dev = own_src, (at(1, core) if in_v else at(0, core)), dev_x
        elif kind == KY:
            src, dst, dev = own_src, (at(2, core) if in_v else at(0, core)), dev_y
        elif kind == KXP:
            src, dst, dev = at(1, core), at(1, core), partner
        elif kind == KYP:
            src, dst, dev = at(2, core), at(2, core), partner
        elif kind == KDY:
            src, dst, dev = at(1, core, 0, half), (at(3, core, 0, half) if in_v else at(1, core, 0, half)), dev_y
        elif kind == KDX:
            src, dst, dev = at(2, core, half, half), (at(3, core, half, half) if in_v else at(2, core, half, half)), dev_x
        elif kind == KDYP:
            src, dst, dev = at(3, core, 0, half), at(3, core, 0, half), partner
        else:
            src, dst, dev = at(3, core, half, half), at(3, core, half, half), partner
        return pltpu.make_async_remote_copy(
            src_ref=src, dst_ref=dst, send_sem=ssem.at[kind, t], recv_sem=rsem.at[kind, t],
            device_id=(dev,), device_id_type=MESH)

    def each(t, body):
        if isinstance(t, int):
            if 0 <= t < pieces:
                body(t < nv)
            return

        @pl.when(t < nv)
        def _():
            body(True)

        @pl.when(jnp.logical_and(t >= nv, t < pieces))
        def _():
            body(False)

    def stage_a(t):
        def body(in_v):
            for kind in (KP, KX, KY):
                copy(kind, t, in_v).start()
        each(t, body)

    def stage_b(t):
        def body(in_v):
            copy(KX, t, in_v).wait_recv()
            copy(KDY, t, in_v).start()
            copy(KXP, t, in_v).start()
            copy(KY, t, in_v).wait_recv()
            copy(KDX, t, in_v).start()
            copy(KYP, t, in_v).start()
        each(t, body)

    def stage_c(t):
        def body(in_v):
            copy(KDY, t, in_v).wait_recv()
            copy(KDYP, t, in_v).start()
            copy(KDX, t, in_v).wait_recv()
            copy(KDXP, t, in_v).start()
        each(t, body)

    def landed(t, kinds):
        each(t, lambda in_v: [copy(kind, t, in_v).wait_recv() for kind in kinds])

    def out_copy(m, col, width, slot):
        half = 0 if width != JW else (m // 2) % 2
        first = 0 if width != JW else pl.multiple_of(half * JW, JW)
        return pltpu.make_async_copy(
            obuf.at[slot, :, pl.ds(first, width)],
            c1_hbm.at[pl.ds(pl.multiple_of(m * BM, BM), BM), pl.ds(col, width)],
            osem.at[slot, half])

    def half_of(m):
        return pl.ds(pl.multiple_of(((m // 2) % 2) * JW, JW), JW)

    def dot(x, y):
        return jnp.dot(x, y, preferred_element_type=F32)

    def pair(i):
        return pl.ds(pl.multiple_of(i * 2 * BM, 2 * BM), 2 * BM)

    def pair_of(place, width):
        x = abuf[:, :, pl.ds(pl.multiple_of(place * slab, slab), width)]
        return x.reshape(2 * BM, width)

    own_v(True).wait()
    stage_a(0)
    stage_a(1)
    for m in range(2, 8):
        a_copy(m, 0, m % 2, m // 2).start()
    own_v(False).start()
    for k in range(2):
        own_h(k, False).start()
    landed(0, (KP,))
    landed(1, (KP,))

    def g0(i, carry):
        for slot in range(2):
            a_copy(2 * i + slot, 0, slot, i).wait()

        @pl.when(i == 2)
        def _():
            for slot in range(2):
                a_copy(slot, 1, slot, 0).start()
                a_copy(slot, 2, slot, 1).start()

        acc[pair(i), :] = dot(pair_of(i, slab), bv[0:slab, 0:JW])
        return carry

    lax.fori_loop(0, nm // 2, g0, 0)
    for k in range(2):
        own_h(k, False).wait()
        own_h(k, True).start()
    stage_b(0)
    stage_b(1)
    stage_a(2)
    stage_a(3)
    landed(0, (KXP, KYP))
    landed(1, (KXP, KYP))

    def g1(i, carry):
        place = 2 * (i % 2)
        for slot in range(2):
            a_copy(2 * i + slot, 1, slot, place).wait()
            a_copy(2 * i + slot, 2, slot, place + 1).wait()

        @pl.when(i < nm // 2 - 1)
        def _():
            for slot in range(2):
                a_copy(2 * i + 2 + slot, 1, slot, 2 - place).start()
                a_copy(2 * i + 2 + slot, 2, slot, 3 - place).start()

        @pl.when(i == 2)
        def _():
            stage_c(0)
            stage_c(1)

        @pl.when(i == 3)
        def _():
            stage_b(2)
            stage_a(4)
            for slot in range(2):
                a_copy(slot, 3, slot, 0).start()
                a_copy(2 + slot, 3, slot, 1).start()

        acc[pair(i), :] += dot(pair_of(place, 2 * slab), bv[slab:3 * slab, 0:JW])
        return carry

    lax.fori_loop(0, nm // 2, g1, 0)
    landed(0, (KDYP, KDXP))
    landed(1, (KDYP, KDXP))
    stage_b(3)
    stage_a(5)
    stage_c(2)
    for k in range(2):
        own_h(k, True).wait()

    def g2(i, carry):
        for slot in range(2):
            a_copy(2 * i + slot, 3, slot, i).wait()

        @pl.when(i == 0)
        def _():
            for slot in range(2):
                a_copy(4 + slot, 3, slot, 2).start()
            a_copy(6, 3, 1, 3).start()
            a_copy(0, 3, 0, 3).start()

        @pl.when(i == 1)
        def _():
            a_copy(0, 0, 0, 0).start()
            a_copy(7, 3, 1, 0).start()

        @pl.when(i == 2)
        def _():
            a_copy(0, 1, 0, 1).start()

        @pl.when(i == 2)
        def _():
            for slot in range(2):
                out_copy(slot, 0, JW, slot).wait()

        res = (acc[pair(i), :] + dot(pair_of(i, slab), bv[3 * slab:, 0:JW])).astype(BF16)
        obuf[:, :, half_of(2 * i)] = res.reshape(2, BM, JW)
        for slot in range(2):
            out_copy(2 * i + slot, 0, JW, slot).start()
        return carry

    lax.fori_loop(0, nm // 2 - 1, g2, 0)
    a_copy(0, 2, 0, 2).start()
    stage_c(3)
    stage_b(4)
    stage_a(6)

    def g2_last(m, carry):
        slot, place = m % 2, 3 * (7 - m)
        a_copy(m, 3, 1, place).wait()
        rows = pl.ds(pl.multiple_of(m * BM, BM), BM)
        out_copy(m - 4, 0, JW, slot).wait()
        obuf[slot, :, half_of(m)] = (acc[rows, :] + dot(
            abuf[1, :, pl.ds(pl.multiple_of(place * slab, slab), slab)], bv[3 * slab:, 0:JW])).astype(BF16)
        out_copy(m, 0, JW, slot).start()
        return carry

    lax.fori_loop(nm - 2, nm, g2_last, 0)

    def tiles(s, m, last):
        slot = s % 2
        for r in range(4):
            a_copy(m, r, slot, r).wait()

        def ahead():
            for r in range(4):
                a_copy((m + 1) % nm, r, 1 - slot, r).start()

        if last is None:
            ahead()
        else:
            pl.when(jnp.logical_not(last))(ahead)
        return slot

    def job1(m, carry):
        slot = tiles(m, m, None)
        h = m // 2

        @pl.when(jnp.logical_and(m % 2 == 0, m > 0))
        def _():
            stage_c(3 + h)

        @pl.when(m % 2 == 1)
        def _():
            stage_b(5 + h)
            stage_a(7 + h)

        @pl.when(m == nm - 1)
        def _():
            stage_c(7)

        @pl.when(m == 0)
        def _():
            for t in (2, 3):
                landed(t, (KP, KXP, KYP, KDYP, KDXP))

        out_copy(m, JW, JW, slot).wait()
        obuf[slot, :, half_of(m)] = dot(abuf[slot], bv[:, JW:2 * JW]).astype(BF16)
        out_copy(m, JW, JW, slot).start()
        return carry

    own_v(False).wait()
    lax.fori_loop(0, nm, job1, 0)
    for t in range(4, 8):
        landed(t, (KP, KXP, KYP, KDYP, KDXP))
    def job2(m, carry):
        slot = tiles(m, m, m == nm - 1)
        stage_b(9 + m)
        stage_a(11 + m)

        @pl.when(m >= 1)
        def _():
            stage_c(7 + m)

        @pl.when(m == nm - 1)
        def _():
            stage_c(15)

        @pl.when(m < 2)
        def _():
            out_copy(m, JW, JW, slot).wait()
            out_copy(m + 2, JW, JW, slot).wait()

        @pl.when(m >= 2)
        def _():
            out_copy(m, 2 * JW, wide, slot).wait()

        obuf[slot] = dot(abuf[slot], bv[:, 2 * JW:]).astype(BF16)
        out_copy(m, 2 * JW, wide, slot).start()
        return carry

    lax.fori_loop(0, nm, job2, 0)

    def rest(t, carry):
        for kind in (KP, KXP, KYP, KDYP, KDXP):
            copy(kind, t, False).wait_recv()
        return carry

    lax.fori_loop(nv, pieces, rest, 0)

    def sent(in_v):
        def body(t, carry):
            for kind in range(9):
                copy(kind, t, in_v).wait_send()
            return carry
        return body

    lax.fori_loop(0, nv, sent(True), 0)
    lax.fori_loop(nv, pieces, sent(False), 0)
    for slot in range(2):
        out_copy(0, 2 * JW, wide, slot).wait()


def _rest_kernel(n1, bn, a_hbm, b_hbm, c1_hbm, c_hbm, abuf, bbuf, obuf, acc, cbuf, asem, bsem, osem, isem, xsem):
    m_rows, k_all = a_hbm.shape
    nm = m_rows // BM
    steps = nm * (b_hbm.shape[1] // bn)
    rows = m_rows // steps
    slab = k_all // 4

    def take(i, k):
        return pltpu.make_async_copy(c1_hbm.at[pl.ds(pl.multiple_of(i * rows, rows), rows), :], cbuf.at[k], isem.at[k])

    def put(i, k):
        return pltpu.make_async_copy(
            cbuf.at[k], c_hbm.at[pl.ds(pl.multiple_of(i * rows, rows), rows), pl.ds(0, n1)], xsem.at[k])

    def out(s, k):
        m, n = s % nm, s // nm
        return pltpu.make_async_copy(
            obuf.at[k],
            c_hbm.at[pl.ds(pl.multiple_of(m * BM, BM), BM), pl.ds(pl.multiple_of(n1 + n * bn, bn), bn)],
            osem.at[k])

    def a_slab(r):
        return pltpu.make_async_copy(
            a_hbm.at[pl.ds(0, BM), pl.ds(pl.multiple_of(r * slab, slab), slab)],
            abuf.at[0, :, pl.ds(pl.multiple_of(r * slab, slab), slab)], asem.at[2 + r])

    def b_slab(r):
        return pltpu.make_async_copy(
            b_hbm.at[pl.ds(pl.multiple_of(r * slab, slab), slab), pl.ds(0, bn)],
            bbuf.at[0, pl.ds(pl.multiple_of(r * slab, slab), slab), :], bsem.at[1 + r])

    def a_tile(s, k):
        return pltpu.make_async_copy(
            a_hbm.at[pl.ds(pl.multiple_of((s % nm) * BM, BM), BM), :], abuf.at[k], asem.at[k])

    b_next = pltpu.make_async_copy(b_hbm.at[:, pl.ds(bn, bn)], bbuf.at[1], bsem.at[0])

    for r in range(4):
        a_slab(r).start()
        b_slab(r).start()
    a_tile(1, 1).start()
    take(0, 0).start()
    acc[...] = jnp.zeros_like(acc)

    def part(r):
        a_slab(r).wait()
        b_slab(r).wait()
        cols = pl.ds(pl.multiple_of(r * slab, slab), slab)
        return jnp.dot(abuf[0, :, cols], bbuf[0, cols, :], preferred_element_type=F32)

    def first(r, carry):
        acc[...] += part(r)
        return carry

    lax.fori_loop(0, 3, first, 0)
    obuf[0] = (acc[...] + part(3)).astype(BF16)
    out(0, 0).start()
    take(0, 0).wait()
    put(0, 0).start()

    def step(s, carry):
        k, c = s % 2, s % 3
        a_tile(s, k).wait()

        @pl.when(s < steps - 1)
        def _():
            a_tile(s + 1, 1 - k).start()

        @pl.when(s == 1)
        def _():
            b_next.start()

        @pl.when(s == nm)
        def _():
            b_next.wait()

        @pl.when(jnp.logical_and(s >= 3, s < steps - 1))
        def _():
            put(s - 3, c).wait()

        @pl.when(s < steps - 1)
        def _():
            take(s, c).start()

        @pl.when(s == steps - 2)
        def _():
            put(steps - 4, (steps - 1) % 3).wait()
            take(steps - 1, (steps - 1) % 3).start()

        @pl.when(s >= 2)
        def _():
            out(s - 2, k).wait()

        obuf[k] = jnp.dot(abuf[k], bbuf[s // nm], preferred_element_type=F32).astype(BF16)
        out(s, k).start()

        @pl.when(s < steps - 1)
        def _():
            take(s, c).wait()
            put(s, c).start()

        @pl.when(s == steps - 2)
        def _():
            take(steps - 1, (steps - 1) % 3).wait()
            put(steps - 1, (steps - 1) % 3).start()
        return carry

    lax.fori_loop(1, steps, step, 0)
    for i in range(steps - 3, steps):
        put(i, i % 3).wait()
    for s in (steps - 2, steps - 1):
        out(s, s % 2).wait()


def solution(mesh):
    def local_fn(a, b):
        m_rows, k_all = a.shape
        depth, n_all = b.shape
        n1 = n_all // 2
        pieces = n_all // CW
        any_spec = pl.BlockSpec(memory_space=pl.ANY)
        c1, bh = pl.pallas_call(
            lambda *refs: _gather_kernel(n1, *refs),
            out_shape=(jax.ShapeDtypeStruct((m_rows, n1), BF16), jax.ShapeDtypeStruct((k_all, n_all - n1), BF16)),
            in_specs=[any_spec, any_spec],
            out_specs=(any_spec, any_spec),
            scratch_shapes=[
                pltpu.VMEM((k_all, n1), BF16),
                pltpu.VMEM((2, BM, k_all), BF16),
                pltpu.VMEM((2, BM, n1 - 2 * JW), BF16),
                pltpu.VMEM((m_rows, JW), F32),
                pltpu.SemaphoreType.DMA((9, pieces)),
                pltpu.SemaphoreType.DMA((9, pieces)),
                pltpu.SemaphoreType.DMA((2, 4)),
                pltpu.SemaphoreType.DMA((2, 2)),
                pltpu.SemaphoreType.DMA((6,)),
            ],
            compiler_params=pltpu.CompilerParams(
                collective_id=0, has_side_effects=True, vmem_limit_bytes=63 * 1024 * 1024),
            cost_estimate=pl.CostEstimate(
                flops=2 * m_rows * k_all * n1, bytes_accessed=6 * m_rows * k_all, transcendentals=0),
            name="gather_half",
        )(a, b)
        bn = 1024
        nm = m_rows // BM
        return pl.pallas_call(
            lambda *refs: _rest_kernel(n1, bn, *refs),
            out_shape=jax.ShapeDtypeStruct((m_rows, n_all), BF16),
            in_specs=[any_spec, any_spec, any_spec],
            out_specs=any_spec,
            scratch_shapes=[
                pltpu.VMEM((2, BM, k_all), BF16),
                pltpu.VMEM((2, k_all, bn), BF16),
                pltpu.VMEM((2, BM, bn), BF16),
                pltpu.VMEM((BM, bn), F32),
                pltpu.VMEM((3, m_rows // (2 * nm), n1), BF16),
                pltpu.SemaphoreType.DMA((6,)),
                pltpu.SemaphoreType.DMA((5,)),
                pltpu.SemaphoreType.DMA((2,)),
                pltpu.SemaphoreType.DMA((3,)),
                pltpu.SemaphoreType.DMA((3,)),
            ],
            compiler_params=pltpu.CompilerParams(vmem_limit_bytes=63 * 1024 * 1024),
            cost_estimate=pl.CostEstimate(
                flops=2 * m_rows * k_all * (n_all - n1), bytes_accessed=6 * m_rows * k_all, transcendentals=0),
            name="rest",
        )(a, bh, c1)

    spec = P("fsdp", None)
    return jax.shard_map(local_fn, mesh=mesh, in_specs=(spec, spec), out_specs=spec, check_vma=False)
```
